32 devices in a mesh: chan: 2 (over x), seq: 16 (over z, y, core).
Axes of the slice: x: 2, y: 2, z: 4, core: 2. Of those that a mesh axis runs over, the one named last changes fastest.
Arguments:
- inputs: bfloat16 [3, 2048, 2, 4096], P(None, 'seq', None, 'chan'), may hold values from -6 to 6
- decay_rate: float32 [4096], P('chan'), may hold values from 0.00024414062 to 0.03
- phase: float32 [4096], P('chan'), may hold values from -3.140625 to 3.140625
- keep: float32 [3, 2048], replicated, may hold values from 0.5 to 1
Outputs:
- states: bfloat16 [3, 2048, 2, 4096], P(None, 'seq', None, 'chan')
The draws below stay inside these ranges and needn't reach their ends.
All inputs are finite; a program needn't handle non-finite values.
Results may differ from the reference program's by a relative error of at most 0.001.
Values sent between devices are 32-bit elements; how exact they have to be, the bound alone decides.
A program may use at most 64 MiB of HBM per device.

```python
import math
import jax
import jax.numpy as jnp
from jax import lax

CHANNELS = 4096
SEQS = 3
SEQ_LEN = 2048


def draw_keep(key, part):
    first_key, second_key = jax.random.split(jax.random.fold_in(key, 11))
    spots = jax.random.randint(first_key, (SEQS, 8), 0, SEQ_LEN)
    levels = jax.random.uniform(second_key, (SEQS, 8), jnp.float32, 0.5, 0.8)
    row_ids = jnp.broadcast_to(jnp.arange(SEQS)[:, None], (SEQS, 8))
    return jnp.ones((SEQS, SEQ_LEN), jnp.float32).at[row_ids, spots].set(levels)


def steps_of(rng, dims, pieces, least, top_value):
    def one(axis_at, blocks):
        steps = jax.random.uniform(jax.random.fold_in(jax.random.fold_in(rng, 6), axis_at), (blocks,), jnp.float32, least / len(pieces), top_value / len(pieces))
        return jnp.repeat(jnp.exp(steps), dims[axis_at] // blocks).reshape((-1,) + (1,) * (len(dims) - axis_at - 1))

    gain = one(*pieces[0])
    for cut in pieces[1:]:
        gain = gain * one(*cut)
    return gain


def normal_values(key, dims, width, bound, cuts=(), kind=jnp.bfloat16):
    values = width * jax.random.normal(key, dims, jnp.float32)
    if cuts:
        values = values * steps_of(key, dims, cuts, -0.22, 0.18)
    return jnp.clip(values, -bound, bound).astype(kind)


def setup_inputs(seed: int = 0) -> dict:
    streams_of = jax.random.split(jax.random.key(seed), 5)
    inputs = normal_values(streams_of[0], (SEQS, SEQ_LEN, 2, CHANNELS), 1.0, 6.0, ((1, 16), (3, 2)))
    decay_rate = jnp.clip(jnp.exp(math.log(0.03) - 4.8112082 * jax.random.uniform(streams_of[1], (CHANNELS,), jnp.float32) ** steps_of(streams_of[1], (CHANNELS,), ((0, 2),), -0.2, 0.2)), 0.00024414062, 0.03)
    phase = jnp.clip(jax.random.uniform(streams_of[2], (CHANNELS,), jnp.float32, -3.140625, 3.140625), -3.140625, 3.140625)
    keep = draw_keep(jax.random.fold_in(streams_of[4], 71), 0)
    return {"inputs": inputs, "decay_rate": decay_rate, "phase": phase, "keep": keep}


def reference(inputs, decay_rate, phase, keep):
    magnitude = jnp.exp(-decay_rate)
    lam_re = magnitude * jnp.cos(phase)
    lam_im = magnitude * jnp.sin(phase)
    gamma = jnp.sqrt(-jnp.expm1(-2.0 * decay_rate))

    def advance(carry, items):
        state_re, state_im = carry
        factor, source_re, source_im = items
        dec_re = factor * lam_re
        dec_im = factor * lam_im
        next_re = dec_re * state_re - dec_im * state_im + source_re
        next_im = dec_re * state_im + dec_im * state_re + source_im
        return ((next_re, next_im), (next_re, next_im))

    def one_sequence(pair):
        sequence, factors = pair
        drive_re = sequence[:, 0, :].astype(jnp.float32) * gamma[None, :]
        drive_im = sequence[:, 1, :].astype(jnp.float32) * gamma[None, :]
        start = (jnp.zeros_like(lam_re), jnp.zeros_like(lam_re))
        _, (all_re, all_im) = lax.scan(advance, start, (factors, drive_re, drive_im))
        return jnp.stack([all_re, all_im], axis=1).astype(jnp.bfloat16)
    return lax.map(one_sequence, (inputs, keep))
```

```python
import functools

import jax
import jax.numpy as jnp
from jax import lax
from jax.experimental import pallas as pl
from jax.experimental.pallas import tpu as pltpu
from jax.sharding import PartitionSpec as P

LANES = 128


def coefficients(decay_rate, phase):
    magnitude = jnp.exp(-decay_rate)
    gamma = jnp.sqrt(-jnp.expm1(-2.0 * decay_rate))
    return (magnitude * jnp.cos(phase), magnitude * jnp.sin(phase), gamma)


def split_view(x):
    b, t, _, c = x.shape
    x = x.reshape(b, t, 2, c // LANES, LANES)
    return x.transpose(0, 1, 3, 2, 4).reshape(b, t, 2 * c // LANES, LANES)


def join_view(x):
    b, t, r, _ = x.shape
    x = x.reshape(b, t, r // 2, 2, LANES)
    return x.transpose(0, 1, 3, 2, 4).reshape(b, t, 2, r * LANES // 2)


def scan_chunk(keep, base, src, lre, lim, gam, state, store):
    batch, steps, rows2, _ = src.shape
    rows = rows2 // 2
    even = pl.ds(0, rows, stride=2)
    odd = pl.ds(1, rows, stride=2)
    for t in range(steps):
        for s in range(batch):
            hre, him = state[s]
            k = keep[s, base + t]
            hre, him = hre * k, him * k
            xre = src[s, t, even, :]
            xim = src[s, t, odd, :]
            if gam is not None:
                xre, xim = xre * gam, xim * gam
            nre = lre * hre - lim * him + xre
            nim = lre * him + lim * hre + xim
            state[s] = (nre, nim)
            if store:
                src[s, t, even, :] = nre
                src[s, t, odd, :] = nim
    return state


def end_kernel(length, keep, x, lre, lim, gam, end, flat, held):
    step = pl.program_id(0)
    batch, steps = x.shape[:2]

    @pl.when(step == 0)
    def _():
        held[...] = jnp.zeros_like(held)

    flat[...] = x[...].astype(jnp.float32)
    base = lax.axis_index("seq") * length + step * steps
    state = [(held[0, s], held[1, s]) for s in range(batch)]
    state = scan_chunk(keep, base, flat, lre[...], lim[...], None, state, False)
    for s in range(batch):
        held[0, s], held[1, s] = state[s]

    @pl.when(step == pl.num_programs(0) - 1)
    def _():
        for s in range(batch):
            end[0, s] = state[s][0] * gam[...]
            end[1, s] = state[s][1] * gam[...]


def full_kernel(length, keep, x, lre, lim, gam, start, out, flat, held):
    step = pl.program_id(0)
    batch, steps = x.shape[:2]

    @pl.when(step == 0)
    def _():
        held[...] = start[...]

    flat[...] = x[...].astype(jnp.float32)
    base = lax.axis_index("seq") * length + step * steps
    state = [(held[0, s], held[1, s]) for s in range(batch)]
    state = scan_chunk(keep, base, flat, lre[...], lim[...], gam[...], state, True)
    for s in range(batch):
        held[0, s], held[1, s] = state[s]
    out[...] = flat[...].astype(jnp.bfloat16)


def shards(inputs, decay_rate, phase, keep):
    lam_re, lam_im, gamma = coefficients(decay_rate, phase)
    batch, length, _, width = inputs.shape
    rows = width // LANES
    lre, lim, gam = (v.reshape(rows, LANES) for v in (lam_re, lam_im, gamma))
    x = split_view(inputs)
    steps = min(16, length)
    grid = (length // steps,)
    whole = pl.BlockSpec(memory_space=pltpu.VMEM)
    smem = pl.BlockSpec(memory_space=pltpu.SMEM)
    block = pl.BlockSpec((batch, steps, 2 * rows, LANES), lambda i: (0, i, 0, 0))
    scratch = [
        pltpu.VMEM((batch, steps, 2 * rows, LANES), jnp.float32),
        pltpu.VMEM((2, batch, rows, LANES), jnp.float32),
    ]
    ends = pl.pallas_call(
        functools.partial(end_kernel, length),
        grid=grid,
        out_shape=jax.ShapeDtypeStruct((2, batch, rows, LANES), jnp.float32),
        in_specs=[smem, block, whole, whole, whole],
        out_specs=whole,
        scratch_shapes=scratch,
        name="ends",
    )(keep, x, lre, lim, gam)

    me = lax.axis_index("seq")
    blocks = lax.axis_size("seq")
    gathered = lax.all_gather(ends[None], "seq", axis=0, tiled=True)
    block_keep = jnp.prod(keep.reshape(batch, blocks, length), axis=2)
    span_mag = jnp.exp(-(length * 1.0) * decay_rate)
    span_re = (span_mag * jnp.cos(length * 1.0 * phase)).reshape(rows, LANES)
    span_im = (span_mag * jnp.sin(length * 1.0 * phase)).reshape(rows, LANES)
    carry_re = jnp.zeros((batch, rows, LANES), jnp.float32)
    carry_im = carry_re
    for b in range(blocks):
        scale = block_keep[:, b][:, None, None]
        tre, tim = scale * span_re, scale * span_im
        nre = tre * carry_re - tim * carry_im + gathered[b, 0]
        nim = tre * carry_im + tim * carry_re + gathered[b, 1]
        carry_re = jnp.where(b < me, nre, carry_re)
        carry_im = jnp.where(b < me, nim, carry_im)
    carry = jnp.stack([carry_re, carry_im])

    out = pl.pallas_call(
        functools.partial(full_kernel, length),
        grid=grid,
        out_shape=jax.ShapeDtypeStruct((batch, length, 2 * rows, LANES), jnp.bfloat16),
        in_specs=[smem, block, whole, whole, whole, whole],
        out_specs=block,
        scratch_shapes=scratch,
        name="full",
    )(keep, x, lre, lim, gam, carry)
    return join_view(out)


def solution(mesh):
    in_specs = (P(None, "seq", None, "chan"), P("chan"), P("chan"), P())
    out_specs = P(None, "seq", None, "chan")
    return jax.shard_map(shards, mesh=mesh, in_specs=in_specs, out_specs=out_specs, check_vma=False)
```

```python
import functools

import jax
import jax.numpy as jnp
from jax import lax
from jax.experimental import pallas as pl
from jax.experimental.pallas import tpu as pltpu
from jax.sharding import PartitionSpec as P

LANES = 128


def coefficients(decay_rate, phase):
    magnitude = jnp.exp(-decay_rate)
    gamma = jnp.sqrt(-jnp.expm1(-2.0 * decay_rate))
    return (magnitude * jnp.cos(phase), magnitude * jnp.sin(phase), gamma)


def split_view(x):
    b, t, _, c = x.shape
    x = x.reshape(b, t, 2, c // LANES, LANES)
    return x.transpose(0, 1, 3, 2, 4).reshape(b, t, 2 * c // LANES, LANES)


def join_view(x):
    b, t, r, _ = x.shape
    x = x.reshape(b, t, r // 2, 2, LANES)
    return x.transpose(0, 1, 3, 2, 4).reshape(b, t, 2, r * LANES // 2)


def scan_chunk(keep, base, src, lre, lim, gam, state, store):
    batch, steps, rows2, _ = src.shape
    rows = rows2 // 2
    even = pl.ds(0, rows, stride=2)
    odd = pl.ds(1, rows, stride=2)
    for t in range(steps):
        for s in range(batch):
            hre, him = state[s]
            k = keep[s, base + t]
            hre, him = hre * k, him * k
            xre = src[s, t, even, :]
            xim = src[s, t, odd, :]
            if gam is not None:
                xre, xim = xre * gam, xim * gam
            nre = lre * hre - lim * him + xre
            nim = lre * him + lim * hre + xim
            state[s] = (nre, nim)
            if store:
                src[s, t, even, :] = nre
                src[s, t, odd, :] = nim
    return state


def cmul(a, b):
    return a[0] * b[0] - a[1] * b[1], a[0] * b[1] + a[1] * b[0]


def exchange(group, blocks, block_keep, span, own, near, total, far, spread, back, sems, carry):
    send_a, recv_a, send_b, recv_b, send_c, recv_c = sems
    batch = own.shape[2]
    me = lax.axis_index("seq")
    part = lax.rem(me, group)
    at = me // group
    groups = blocks // group

    def member(d):
        return lax.rem(part + d, group)

    def copy(src, dst, send, recv, target):
        return pltpu.make_async_remote_copy(
            src_ref=src, dst_ref=dst, send_sem=send, recv_sem=recv,
            device_id={"seq": target}, device_id_type=pl.DeviceIdType.MESH,
        )

    def copy_a(d):
        return copy(own.at[member(d)], near.at[d], send_a.at[d], recv_a.at[d], at * group + member(d))

    def copy_b(d):
        return copy(total, far.at[d], send_b.at[d], recv_b.at[d], me + d * group)

    def copy_c(d):
        return copy(spread.at[d], back.at[d], send_c.at[d], recv_c.at[d], at * group + member(d))

    for d in range(group - 1, 0, -1):
        copy_a(d).start()
    near[0] = own[part]
    lam = (span[part, 0], span[part, 1])
    powers = [None, lam]
    for _ in range(group - 1):
        powers.append(cmul(powers[-1], lam))
    for d in range(1, group):
        copy_a(d).wait_recv()

    inner = [[None] * batch for _ in range(group + 1)]
    scales = [[None] * batch for _ in range(group + 1)]
    for i in range(group):
        slot = lax.rem(part + group - i, group)
        for s in range(batch):
            k = block_keep[s, at * group + i]
            end = (near[slot, 0, s], near[slot, 1, s])
            if i == 0:
                inner[1][s], scales[1][s] = end, k
            else:
                step = cmul((k * lam[0], k * lam[1]), inner[i][s])
                inner[i + 1][s] = (step[0] + end[0], step[1] + end[1])
                scales[i + 1][s] = scales[i][s] * k
    for s in range(batch):
        total[0, s], total[1, s] = inner[group][s]
    for d in range(groups - 1, 0, -1):

        @pl.when(at + d < groups)
        def _(d=d):
            copy_b(d).start()

    for m in range(group):
        slot = lax.rem(m + group - part, group)
        for s in range(batch):
            if m == 0:
                zero = jnp.zeros_like(lam[0])
                spread[slot, 0, s], spread[slot, 1, s] = zero, zero
            else:
                spread[slot, 0, s], spread[slot, 1, s] = inner[m][s]
    far[0] = jnp.zeros(far.shape[1:], jnp.float32)
    for d in range(groups - 1, 0, -1):

        @pl.when(at - d >= 0)
        def _(d=d):
            copy_b(d).wait_recv()
            for s in range(batch):
                k = jnp.float32(1)
                for i in range(group):
                    k = k * block_keep[s, (at - d) * group + i]
                step = cmul((k * powers[group][0], k * powers[group][1]), (far[0, 0, s], far[0, 1, s]))
                far[0, 0, s] = step[0] + far[d, 0, s]
                far[0, 1, s] = step[1] + far[d, 1, s]

    entry = [(far[0, 0, s], far[0, 1, s]) for s in range(batch)]
    for m in range(group):
        slot = lax.rem(m + group - part, group)
        for s in range(batch):
            if m == 0:
                step = entry[s]
            else:
                step = cmul((scales[m][s] * powers[m][0], scales[m][s] * powers[m][1]), entry[s])
            spread[slot, 0, s] += step[0]
            spread[slot, 1, s] += step[1]
    for d in range(group - 1, 0, -1):
        copy_c(d).start()
    carry[part] = spread[0]
    for d in range(1, group):
        copy_c(d).wait_recv()
        carry[lax.rem(part + group - d, group)] = back[d]
    for d in range(1, group):
        copy_a(d).wait_send()
        copy_c(d).wait_send()
    for d in range(1, groups):

        @pl.when(at + d < groups)
        def _(d=d):
            copy_b(d).wait_send()


def end_kernel(length, group, blocks, keep, block_keep, x, lre, lim, gam, span, carry, flat, held, own, near, total, far, spread, back, *sems):
    step = pl.program_id(0)
    batch, steps = x.shape[:2]
    me = lax.axis_index("seq")
    barrier = pltpu.get_barrier_semaphore()
    peers = group - 1 + blocks // group - 1

    @pl.when(step == 0)
    def _():
        held[...] = jnp.zeros_like(held)
        first = me // group * group
        for d in range(1, group):
            peer = first + lax.rem(me + d, group)
            pl.semaphore_signal(barrier, inc=1, device_id={"seq": peer}, device_id_type=pl.DeviceIdType.MESH)
        for d in range(1, blocks // group):
            peer = lax.rem(me + d * group, blocks)
            pl.semaphore_signal(barrier, inc=1, device_id={"seq": peer}, device_id_type=pl.DeviceIdType.MESH)

    flat[...] = x[...].astype(jnp.float32)
    base = me * length + step * steps
    state = [(held[0, s], held[1, s]) for s in range(batch)]
    state = scan_chunk(keep, base, flat, lre[...], lim[...], None, state, False)
    for s in range(batch):
        held[0, s], held[1, s] = state[s]

    @pl.when(step == pl.num_programs(0) - 1)
    def _():
        part_rows = own.shape[3]
        for s in range(batch):
            for c in range(2):
                value = state[s][c] * gam[...]
                for p in range(group):
                    own[p, c, s] = value[p * part_rows : (p + 1) * part_rows]
        pl.semaphore_wait(barrier, peers)
        exchange(group, blocks, block_keep, span, own, near, total, far, spread, back, sems, carry)


def full_kernel(length, keep, x, lre, lim, gam, start, out, flat, held):
    step = pl.program_id(0)
    batch, steps = x.shape[:2]

    @pl.when(step == 0)
    def _():
        group, _, _, part_rows, _ = start.shape
        for p in range(group):
            held[:, :, p * part_rows : (p + 1) * part_rows] = start[p]

    flat[...] = x[...].astype(jnp.float32)
    base = lax.axis_index("seq") * length + step * steps
    state = [(held[0, s], held[1, s]) for s in range(batch)]
    state = scan_chunk(keep, base, flat, lre[...], lim[...], gam[...], state, True)
    for s in range(batch):
        held[0, s], held[1, s] = state[s]
    out[...] = flat[...].astype(jnp.bfloat16)


def shards(inputs, decay_rate, phase, keep):
    lam_re, lam_im, gamma = coefficients(decay_rate, phase)
    batch, length, _, width = inputs.shape
    rows = width // LANES
    lre, lim, gam = (v.reshape(rows, LANES) for v in (lam_re, lam_im, gamma))
    x = split_view(inputs)
    steps = min(16, length)
    grid = (length // steps,)
    whole = pl.BlockSpec(memory_space=pltpu.VMEM)
    smem = pl.BlockSpec(memory_space=pltpu.SMEM)
    block = pl.BlockSpec((batch, steps, 2 * rows, LANES), lambda i: (0, i, 0, 0))
    scratch = [
        pltpu.VMEM((batch, steps, 2 * rows, LANES), jnp.float32),
        pltpu.VMEM((2, batch, rows, LANES), jnp.float32),
    ]
    blocks = lax.axis_size("seq")
    group = 4
    groups = blocks // group
    block_keep = jnp.prod(keep.reshape(batch, blocks, length), axis=2)
    span_mag = jnp.exp(-(length * 1.0) * decay_rate)
    span_re = (span_mag * jnp.cos(length * 1.0 * phase)).reshape(group, rows // group, LANES)
    span_im = (span_mag * jnp.sin(length * 1.0 * phase)).reshape(group, rows // group, LANES)
    span = jnp.stack([span_re, span_im], axis=1)
    piece = (2, batch, rows // group, LANES)
    dma = pltpu.SemaphoreType.DMA
    carry = pl.pallas_call(
        functools.partial(end_kernel, length, group, blocks),
        grid=grid,
        out_shape=jax.ShapeDtypeStruct((group,) + piece, jnp.float32),
        in_specs=[smem, smem, block, whole, whole, whole, whole],
        out_specs=whole,
        scratch_shapes=scratch
        + [
            pltpu.VMEM((group,) + piece, jnp.float32),
            pltpu.VMEM((group,) + piece, jnp.float32),
            pltpu.VMEM(piece, jnp.float32),
            pltpu.VMEM((groups,) + piece, jnp.float32),
            pltpu.VMEM((group,) + piece, jnp.float32),
            pltpu.VMEM((group,) + piece, jnp.float32),
            dma((group,)), dma((group,)), dma((groups,)), dma((groups,)), dma((group,)), dma((group,)),
        ],
        compiler_params=pltpu.CompilerParams(collective_id=0, has_side_effects=True),
        name="ends",
    )(keep, block_keep, x, lre, lim, gam, span)

    out = pl.pallas_call(
        functools.partial(full_kernel, length),
        grid=grid,
        out_shape=jax.ShapeDtypeStruct((batch, length, 2 * rows, LANES), jnp.bfloat16),
        in_specs=[smem, block, whole, whole, whole, whole],
        out_specs=block,
        scratch_shapes=scratch,
        name="full",
    )(keep, x, lre, lim, gam, carry)
    return join_view(out)


def solution(mesh):
    in_specs = (P(None, "seq", None, "chan"), P("chan"), P("chan"), P())
    out_specs = P(None, "seq", None, "chan")
    return jax.shard_map(shards, mesh=mesh, in_specs=in_specs, out_specs=out_specs, check_vma=False)
```

```python
import functools

import jax
import jax.numpy as jnp
from jax import lax
from jax.experimental import pallas as pl
from jax.experimental.pallas import tpu as pltpu
from jax.sharding import PartitionSpec as P

LANES = 128
GRANT = 12 * 1024 * 1024


def coefficients(decay_rate, phase):
    magnitude = jnp.exp(-decay_rate)
    y = 2.0 * decay_rate
    series = 1.0 - y / 6.0 * (1.0 - y / 7.0)
    for n in (5.0, 4.0, 3.0, 2.0):
        series = 1.0 - y / n * series
    gamma = jnp.sqrt(jnp.where(y < 0.0625, y * series, 1.0 - jnp.exp(-y)))
    return (magnitude * jnp.cos(phase), magnitude * jnp.sin(phase), gamma)


def split_view(x):
    b, t, _, c = x.shape
    x = x.reshape(b, t, 2, c // LANES, LANES)
    return x.transpose(0, 1, 3, 2, 4).reshape(b, t, 2 * c // LANES, LANES)


def join_view(x):
    b, t, r, _ = x.shape
    x = x.reshape(b, t, r // 2, 2, LANES)
    return x.transpose(0, 1, 3, 2, 4).reshape(b, t, 2, r * LANES // 2)


def scan_chunk(keep, base, src, lre, lim, gam, state, store):
    batch, steps, rows2, _ = src.shape
    rows = rows2 // 2
    even = pl.ds(0, rows, stride=2)
    odd = pl.ds(1, rows, stride=2)
    for t in range(steps):
        for s in range(batch):
            hre, him = state[s]
            k = keep[s, base + t]
            hre, him = hre * k, him * k
            xre = src[s, t, even, :]
            xim = src[s, t, odd, :]
            if gam is not None:
                xre, xim = xre * gam, xim * gam
            nre = lre * hre - lim * him + xre
            nim = lre * him + lim * hre + xim
            state[s] = (nre, nim)
            if store:
                src[s, t, even, :] = nre
                src[s, t, odd, :] = nim
    return state


def cmul(a, b):
    return a[0] * b[0] - a[1] * b[1], a[0] * b[1] + a[1] * b[0]


def exchange(length, group, blocks, keep_rows, coef, prods, span, own, near, total, far, spread, back, sems, carry):
    send_a, recv_a, send_b, recv_b, send_c, recv_c = sems
    batch = own.shape[2]
    me = lax.axis_index("seq")
    part = lax.rem(me, group)
    at = me // group
    groups = blocks // group

    def member(d):
        return lax.rem(part + d, group)

    def copy(src, dst, send, recv, target):
        return pltpu.make_async_remote_copy(
            src_ref=src, dst_ref=dst, send_sem=send, recv_sem=recv,
            device_id={"seq": target}, device_id_type=pl.DeviceIdType.MESH,
        )

    def copy_a(d):
        return copy(own.at[member(d)], near.at[d], send_a.at[d], recv_a.at[d], at * group + member(d))

    def copy_b(d):
        return copy(total, far.at[d], send_b.at[d], recv_b.at[d], me + d * group)

    def copy_c(d):
        return copy(spread.at[d], back.at[d], send_c.at[d], recv_c.at[d], at * group + member(d))

    for d in range(group - 1, 0, -1):
        copy_a(d).start()
    near[0] = own[part]
    power = (coef[0], coef[1])
    done, left = None, length
    while left:
        if left % 2:
            done = power if done is None else cmul(done, power)
        left //= 2
        if left:
            power = cmul(power, power)
    part_rows = own.shape[3]
    for p in range(group):
        for c in range(2):
            span[p, c] = done[c][p * part_rows : (p + 1) * part_rows]
    for b in range(blocks):
        logs = jnp.log(keep_rows[:, b * length : (b + 1) * length])
        prods[b] = jnp.broadcast_to(jnp.exp(jnp.sum(logs, axis=1, keepdims=True)), prods.shape[1:])
    lam = (span[part, 0], span[part, 1])
    powers = [None, lam]
    for _ in range(group - 1):
        powers.append(cmul(powers[-1], lam))
    for d in range(1, group):
        copy_a(d).wait_recv()

    inner = [[None] * batch for _ in range(group + 1)]
    scales = [[None] * batch for _ in range(group + 1)]
    for i in range(group):
        slot = lax.rem(part + group - i, group)
        for s in range(batch):
            k = prods[at * group + i, pl.ds(s, 1), :]
            end = (near[slot, 0, s], near[slot, 1, s])
            if i == 0:
                inner[1][s], scales[1][s] = end, k
            else:
                step = cmul((k * lam[0], k * lam[1]), inner[i][s])
                inner[i + 1][s] = (step[0] + end[0], step[1] + end[1])
                scales[i + 1][s] = scales[i][s] * k
    for s in range(batch):
        total[0, s], total[1, s] = inner[group][s]
    for d in range(groups - 1, 0, -1):

        @pl.when(at + d < groups)
        def _(d=d):
            copy_b(d).start()

    for m in range(group):
        slot = lax.rem(m + group - part, group)
        for s in range(batch):
            if m == 0:
                zero = jnp.zeros_like(lam[0])
                spread[slot, 0, s], spread[slot, 1, s] = zero, zero
            else:
                spread[slot, 0, s], spread[slot, 1, s] = inner[m][s]
    far[0] = jnp.zeros(far.shape[1:], jnp.float32)
    for d in range(groups - 1, 0, -1):

        @pl.when(at - d >= 0)
        def _(d=d):
            copy_b(d).wait_recv()
            for s in range(batch):
                k = prods[(at - d) * group, pl.ds(s, 1), :]
                for i in range(1, group):
                    k = k * prods[(at - d) * group + i, pl.ds(s, 1), :]
                step = cmul((k * powers[group][0], k * powers[group][1]), (far[0, 0, s], far[0, 1, s]))
                far[0, 0, s] = step[0] + far[d, 0, s]
                far[0, 1, s] = step[1] + far[d, 1, s]

    entry = [(far[0, 0, s], far[0, 1, s]) for s in range(batch)]
    for m in range(group):
        slot = lax.rem(m + group - part, group)
        for s in range(batch):
            if m == 0:
                step = entry[s]
            else:
                step = cmul((scales[m][s] * powers[m][0], scales[m][s] * powers[m][1]), entry[s])
            spread[slot, 0, s] += step[0]
            spread[slot, 1, s] += step[1]
    for d in range(group - 1, 0, -1):
        copy_c(d).start()
    carry[part] = spread[0]
    for d in range(1, group):
        copy_c(d).wait_recv()
        carry[lax.rem(part + group - d, group)] = back[d]
    for d in range(1, group):
        copy_a(d).wait_send()
        copy_c(d).wait_send()
    for d in range(1, groups):

        @pl.when(at + d < groups)
        def _(d=d):
            copy_b(d).wait_send()


def end_kernel(length, group, blocks, keep, keep_rows, x, decay, phase, carry, coef, flat, held, prods, span, own, near, total, far, spread, back, *sems):
    step = pl.program_id(0)
    batch, steps = x.shape[:2]
    me = lax.axis_index("seq")
    barrier = pltpu.get_barrier_semaphore()
    peers = group - 1 + blocks // group - 1

    @pl.when(step == 0)
    def _():
        held[...] = jnp.zeros_like(held)
        coef[0], coef[1], coef[2] = coefficients(decay[...], phase[...])
        first = me // group * group
        for d in range(1, group):
            peer = first + lax.rem(me + d, group)
            pl.semaphore_signal(barrier, inc=1, device_id={"seq": peer}, device_id_type=pl.DeviceIdType.MESH)
        for d in range(1, blocks // group):
            peer = lax.rem(me + d * group, blocks)
            pl.semaphore_signal(barrier, inc=1, device_id={"seq": peer}, device_id_type=pl.DeviceIdType.MESH)

    flat[...] = x[...].astype(jnp.float32)
    base = me * length + step * steps
    state = [(held[0, s], held[1, s]) for s in range(batch)]
    state = scan_chunk(keep, base, flat, coef[0], coef[1], None, state, False)
    for s in range(batch):
        held[0, s], held[1, s] = state[s]

    @pl.when(step == pl.num_programs(0) - 1)
    def _():
        part_rows = own.shape[3]
        for s in range(batch):
            for c in range(2):
                value = state[s][c] * coef[2]
                for p in range(group):
                    own[p, c, s] = value[p * part_rows : (p + 1) * part_rows]
        pl.semaphore_wait(barrier, peers)
        exchange(length, group, blocks, keep_rows, coef, prods, span, own, near, total, far, spread, back, sems, carry)


def full_kernel(length, keep, x, coef, start, out, flat, held):
    step = pl.program_id(0)
    batch, steps = x.shape[:2]

    @pl.when(step == 0)
    def _():
        group, _, _, part_rows, _ = start.shape
        for p in range(group):
            held[:, :, p * part_rows : (p + 1) * part_rows] = start[p]

    flat[...] = x[...].astype(jnp.float32)
    base = lax.axis_index("seq") * length + step * steps
    state = [(held[0, s], held[1, s]) for s in range(batch)]
    state = scan_chunk(keep, base, flat, coef[0], coef[1], coef[2], state, True)
    for s in range(batch):
        held[0, s], held[1, s] = state[s]
    out[...] = flat[...].astype(jnp.bfloat16)


def shards(inputs, decay_rate, phase, keep):
    batch, length, _, width = inputs.shape
    rows = width // LANES
    x = split_view(inputs)
    steps = min(16, length)
    grid = (length // steps,)
    whole = pl.BlockSpec(memory_space=pltpu.VMEM)
    smem = pl.BlockSpec(memory_space=pltpu.SMEM)
    block = pl.BlockSpec((batch, steps, 2 * rows, LANES), lambda i: (0, i, 0, 0))
    scratch = [
        pltpu.VMEM((batch, steps, 2 * rows, LANES), jnp.float32),
        pltpu.VMEM((2, batch, rows, LANES), jnp.float32),
    ]
    blocks = lax.axis_size("seq")
    group = 4
    groups = blocks // group
    piece = (2, batch, rows // group, LANES)
    dma = pltpu.SemaphoreType.DMA
    carry, coef = pl.pallas_call(
        functools.partial(end_kernel, length, group, blocks),
        grid=grid,
        out_shape=(
            jax.ShapeDtypeStruct((group,) + piece, jnp.float32),
            jax.ShapeDtypeStruct((3, rows, LANES), jnp.float32),
        ),
        in_specs=[smem, whole, block, whole, whole],
        out_specs=(whole, whole),
        scratch_shapes=scratch
        + [
            pltpu.VMEM((blocks, batch, LANES), jnp.float32),
            pltpu.VMEM((group, 2, rows // group, LANES), jnp.float32),
            pltpu.VMEM((group,) + piece, jnp.float32),
            pltpu.VMEM((group,) + piece, jnp.float32),
            pltpu.VMEM(piece, jnp.float32),
            pltpu.VMEM((groups,) + piece, jnp.float32),
            pltpu.VMEM((group,) + piece, jnp.float32),
            pltpu.VMEM((group,) + piece, jnp.float32),
            dma((group,)), dma((group,)), dma((groups,)), dma((groups,)), dma((group,)), dma((group,)),
        ],
        compiler_params=pltpu.CompilerParams(collective_id=0, has_side_effects=True, vmem_limit_bytes=GRANT),
        name="ends",
    )(keep, keep, x, decay_rate.reshape(rows, LANES), phase.reshape(rows, LANES))

    out = pl.pallas_call(
        functools.partial(full_kernel, length),
        grid=grid,
        out_shape=jax.ShapeDtypeStruct((batch, length, 2 * rows, LANES), jnp.bfloat16),
        in_specs=[smem, block, whole, whole],
        out_specs=block,
        scratch_shapes=scratch,
        compiler_params=pltpu.CompilerParams(vmem_limit_bytes=GRANT),
        name="full",
    )(keep, x, coef, carry)
    return join_view(out)


def solution(mesh):
    in_specs = (P(None, "seq", None, "chan"), P("chan"), P("chan"), P())
    out_specs = P(None, "seq", None, "chan")
    return jax.shard_map(shards, mesh=mesh, in_specs=in_specs, out_specs=out_specs, check_vma=False)
```

```python
import functools

import jax
import jax.numpy as jnp
from jax import lax
from jax.experimental import pallas as pl
from jax.experimental.pallas import tpu as pltpu
from jax.sharding import PartitionSpec as P

LANES = 128
GRANT = 12 * 1024 * 1024


def coefficients(decay_rate, phase):
    magnitude = jnp.exp(-decay_rate)
    y = 2.0 * decay_rate
    series = 1.0 - y / 6.0 * (1.0 - y / 7.0)
    for n in (5.0, 4.0, 3.0, 2.0):
        series = 1.0 - y / n * series
    gamma = jnp.sqrt(jnp.where(y < 0.0625, y * series, 1.0 - jnp.exp(-y)))
    return (magnitude * jnp.cos(phase), magnitude * jnp.sin(phase), gamma)


def split_view(x):
    b, t, _, c = x.shape
    x = x.reshape(b, t, 2, c // LANES, LANES)
    return x.transpose(0, 1, 3, 2, 4).reshape(b, t, 2 * c // LANES, LANES)


def join_view(x):
    b, t, r, _ = x.shape
    x = x.reshape(b, t, r // 2, 2, LANES)
    return x.transpose(0, 1, 3, 2, 4).reshape(b, t, 2, r * LANES // 2)


def scan_chunk(keep, base, src, lre, lim, gam, state, store):
    batch, steps, rows2, _ = src.shape
    rows = rows2 // 2
    even = pl.ds(0, rows, stride=2)
    odd = pl.ds(1, rows, stride=2)
    for t in range(steps):
        for s in range(batch):
            hre, him = state[s]
            k = keep[s, base + t]
            hre, him = hre * k, him * k
            xre = src[s, t, even, :]
            xim = src[s, t, odd, :]
            if gam is not None:
                xre, xim = xre * gam, xim * gam
            nre = lre * hre - lim * him + xre
            nim = lre * him + lim * hre + xim
            state[s] = (nre, nim)
            if store:
                src[s, t, even, :] = nre
                src[s, t, odd, :] = nim
    return state


def cmul(a, b):
    return a[0] * b[0] - a[1] * b[1], a[0] * b[1] + a[1] * b[0]


def exchange(length, group, blocks, keep_rows, coef, prods, span, own, near, total, far, spread, back, sems, carry, fill_a, fill_b):
    send_a, recv_a, send_b, recv_b, send_c, recv_c = sems
    batch = own.shape[2]
    me = lax.axis_index("seq")
    part = lax.rem(me, group)
    at = me // group
    groups = blocks // group

    def member(d):
        return lax.rem(part + d, group)

    def copy(src, dst, send, recv, target):
        return pltpu.make_async_remote_copy(
            src_ref=src, dst_ref=dst, send_sem=send, recv_sem=recv,
            device_id={"seq": target}, device_id_type=pl.DeviceIdType.MESH,
        )

    def copy_a(d):
        return copy(own.at[member(d)], near.at[d], send_a.at[d], recv_a.at[d], at * group + member(d))

    def copy_b(d):
        return copy(total, far.at[d], send_b.at[d], recv_b.at[d], me + d * group)

    def copy_c(d):
        return copy(spread.at[d], back.at[d], send_c.at[d], recv_c.at[d], at * group + member(d))

    for d in range(group - 1, 0, -1):
        copy_a(d).start()
    near[0] = own[part]
    power = (coef[0], coef[1])
    done, left = None, length
    while left:
        if left % 2:
            done = power if done is None else cmul(done, power)
        left //= 2
        if left:
            power = cmul(power, power)
    part_rows = own.shape[3]
    for p in range(group):
        for c in range(2):
            span[p, c] = done[c][p * part_rows : (p + 1) * part_rows]
    for b in range(blocks):
        logs = jnp.log(keep_rows[:, b * length : (b + 1) * length])
        prods[b] = jnp.broadcast_to(jnp.exp(jnp.sum(logs, axis=1, keepdims=True)), prods.shape[1:])
    lam = (span[part, 0], span[part, 1])
    fill_a()
    powers = [None, lam]
    for _ in range(group - 1):
        powers.append(cmul(powers[-1], lam))
    for d in range(1, group):
        copy_a(d).wait_recv()

    inner = [[None] * batch for _ in range(group + 1)]
    scales = [[None] * batch for _ in range(group + 1)]
    for i in range(group):
        slot = lax.rem(part + group - i, group)
        for s in range(batch):
            k = prods[at * group + i, pl.ds(s, 1), :]
            end = (near[slot, 0, s], near[slot, 1, s])
            if i == 0:
                inner[1][s], scales[1][s] = end, k
            else:
                step = cmul((k * lam[0], k * lam[1]), inner[i][s])
                inner[i + 1][s] = (step[0] + end[0], step[1] + end[1])
                scales[i + 1][s] = scales[i][s] * k
    for s in range(batch):
        total[0, s], total[1, s] = inner[group][s]
    for d in range(groups - 1, 0, -1):

        @pl.when(at + d < groups)
        def _(d=d):
            copy_b(d).start()

    for m in range(group):
        slot = lax.rem(m + group - part, group)
        for s in range(batch):
            if m == 0:
                zero = jnp.zeros_like(lam[0])
                spread[slot, 0, s], spread[slot, 1, s] = zero, zero
            else:
                spread[slot, 0, s], spread[slot, 1, s] = inner[m][s]
    far[0] = jnp.zeros(far.shape[1:], jnp.float32)
    fill_b()
    for d in range(groups - 1, 0, -1):

        @pl.when(at - d >= 0)
        def _(d=d):
            copy_b(d).wait_recv()
            for s in range(batch):
                k = prods[(at - d) * group, pl.ds(s, 1), :]
                for i in range(1, group):
                    k = k * prods[(at - d) * group + i, pl.ds(s, 1), :]
                step = cmul((k * powers[group][0], k * powers[group][1]), (far[0, 0, s], far[0, 1, s]))
                far[0, 0, s] = step[0] + far[d, 0, s]
                far[0, 1, s] = step[1] + far[d, 1, s]

    entry = [(far[0, 0, s], far[0, 1, s]) for s in range(batch)]
    for m in range(group):
        slot = lax.rem(m + group - part, group)
        for s in range(batch):
            if m == 0:
                step = entry[s]
            else:
                step = cmul((scales[m][s] * powers[m][0], scales[m][s] * powers[m][1]), entry[s])
            spread[slot, 0, s] += step[0]
            spread[slot, 1, s] += step[1]
    for d in range(group - 1, 0, -1):
        copy_c(d).start()
    carry[part] = spread[0]
    for d in range(1, group):
        copy_c(d).wait_recv()
        carry[lax.rem(part + group - d, group)] = back[d]
    for d in range(1, group):
        copy_a(d).wait_send()
        copy_c(d).wait_send()
    for d in range(1, groups):

        @pl.when(at + d < groups)
        def _(d=d):
            copy_b(d).wait_send()


def end_kernel(length, group, blocks, steps, keep_hbm, x_hbm, decay_hbm, phase_hbm, states, table, entry,
               x, keep, keep_rows, decay, phase, coef, twice, prods, span, own, near, total, far, spread, back, carry,
               x_sem, small_sem, *sems):
    batch = states.shape[0]
    rows = coef.shape[1]
    chunks = length // steps
    even = pl.ds(0, rows, stride=2)
    odd = pl.ds(1, rows, stride=2)
    small = [
        pltpu.make_async_copy(src, dst, small_sem.at[i])
        for i, (src, dst) in enumerate(
            ((decay_hbm, decay), (phase_hbm, phase), (keep_hbm, keep), (keep_hbm, keep_rows))
        )
    ]

    def load(i):
        at = pl.ds(i * steps, steps)
        return pltpu.make_async_copy(x_hbm.at[:, at], x.at[:, at], x_sem.at[i])

    for copy in small[:3]:
        copy.start()
    for i in range(chunks):
        load(i).start()
    small[3].start()

    me = lax.axis_index("seq")
    barrier = pltpu.get_barrier_semaphore()
    first = me // group * group
    for d in range(1, group):
        peer = first + lax.rem(me + d, group)
        pl.semaphore_signal(barrier, inc=1, device_id={"seq": peer}, device_id_type=pl.DeviceIdType.MESH)
    for d in range(1, blocks // group):
        peer = lax.rem(me + d * group, blocks)
        pl.semaphore_signal(barrier, inc=1, device_id={"seq": peer}, device_id_type=pl.DeviceIdType.MESH)

    small[0].wait()
    small[1].wait()
    coef[0], coef[1], coef[2] = coefficients(decay[...], phase[...])
    for c in range(2):
        twice[c, even, :] = coef[c]
        twice[c, odd, :] = coef[c]
    small[2].wait()
    base = me * length
    zero = jnp.zeros((rows, LANES), jnp.float32)
    start = tuple((zero, zero) for _ in range(batch))

    def ends(i, state):
        at = pl.ds(i * steps, steps)
        load(i).wait()
        states[:, at] = x[:, at].astype(jnp.float32)
        state = scan_chunk(keep, base + i * steps, states.at[:, at], coef[0], coef[1], None, list(state), False)
        return tuple(state)

    state = lax.fori_loop(0, chunks, ends, start)
    part_rows = own.shape[3]
    for s in range(batch):
        for c in range(2):
            value = state[s][c] * coef[2]
            for p in range(group):
                own[p, c, s] = value[p * part_rows : (p + 1) * part_rows]

    def fill_a():
        ones = jnp.ones((2 * rows, LANES), jnp.float32)

        def powers(i, held):
            power, scale = held
            scale = list(scale)
            for t in range(4):
                power = cmul((twice[0], twice[1]), power)
                for s in range(batch):
                    scale[s] = scale[s] * keep[s, base + i * 4 + t]
                    table[s, i * 4 + t, 0] = scale[s] * power[0]
                    table[s, i * 4 + t, 1] = scale[s] * power[1]
            return power, tuple(scale)

        unit = tuple(jnp.float32(1) for _ in range(batch))
        lax.fori_loop(0, length // 4, powers, ((ones, jnp.zeros_like(ones)), unit))

    def fill_b():
        def local(i, state):
            at = pl.ds(i * steps, steps)
            view = states.at[:, at]
            return tuple(scan_chunk(keep, base + i * steps, view, coef[0], coef[1], coef[2], list(state), True))

        lax.fori_loop(0, chunks, local, start)

    small[3].wait()
    pl.semaphore_wait(barrier, group - 1 + blocks // group - 1)
    exchange(length, group, blocks, keep_rows, coef, prods, span, own, near, total, far, spread, back, sems, carry,
             fill_a, fill_b)
    for s in range(batch):
        for p in range(group):
            top = pl.ds(2 * p * part_rows, part_rows, stride=2)
            low = pl.ds(2 * p * part_rows + 1, part_rows, stride=2)
            entry[s, 0, top, :] = carry[p, 0, s]
            entry[s, 0, low, :] = carry[p, 1, s]
            entry[s, 1, top, :] = -carry[p, 1, s]
            entry[s, 1, low, :] = carry[p, 0, s]


def full_kernel(states, table, entry, out):
    batch, steps = out.shape[:2]
    base = pl.program_id(0) * steps
    for s in range(batch):
        for t in range(steps):
            at = base + t
            moved = table[s, at, 0] * entry[s, 0] + table[s, at, 1] * entry[s, 1]
            out[s, t] = (states[s, at] + moved).astype(jnp.bfloat16)


def shards(inputs, decay_rate, phase, keep):
    batch, length, _, width = inputs.shape
    rows = width // LANES
    x = split_view(inputs)
    steps = min(16, length)
    chunks = length // steps
    blocks = lax.axis_size("seq")
    group = 4
    groups = blocks // group
    whole = pl.BlockSpec(memory_space=pltpu.VMEM)
    away = pl.BlockSpec(memory_space=pltpu.HBM)
    piece = (2, batch, rows // group, LANES)
    dma = pltpu.SemaphoreType.DMA
    f32 = jnp.float32
    states, table, entry = pl.pallas_call(
        functools.partial(end_kernel, length, group, blocks, steps),
        out_shape=(
            jax.ShapeDtypeStruct((batch, length, 2 * rows, LANES), f32),
            jax.ShapeDtypeStruct((batch, length, 2, 2 * rows, LANES), f32),
            jax.ShapeDtypeStruct((batch, 2, 2 * rows, LANES), f32),
        ),
        in_specs=[away] * 4,
        out_specs=(whole,) * 3,
        scratch_shapes=[
            pltpu.VMEM((batch, length, 2 * rows, LANES), jnp.bfloat16),
            pltpu.SMEM(keep.shape, f32),
            pltpu.VMEM(keep.shape, f32),
            pltpu.VMEM((rows, LANES), f32),
            pltpu.VMEM((rows, LANES), f32),
            pltpu.VMEM((3, rows, LANES), f32),
            pltpu.VMEM((2, 2 * rows, LANES), f32),
            pltpu.VMEM((blocks, batch, LANES), f32),
            pltpu.VMEM((group, 2, rows // group, LANES), f32),
            pltpu.VMEM((group,) + piece, f32),
            pltpu.VMEM((group,) + piece, f32),
            pltpu.VMEM(piece, f32),
            pltpu.VMEM((groups,) + piece, f32),
            pltpu.VMEM((group,) + piece, f32),
            pltpu.VMEM((group,) + piece, f32),
            pltpu.VMEM((group,) + piece, f32),
            dma((chunks,)), dma((4,)),
            dma((group,)), dma((group,)), dma((groups,)), dma((groups,)), dma((group,)), dma((group,)),
        ],
        compiler_params=pltpu.CompilerParams(collective_id=0, has_side_effects=True, vmem_limit_bytes=GRANT),
        name="ends",
    )(keep, x, decay_rate.reshape(rows, LANES), phase.reshape(rows, LANES))
    out = pl.pallas_call(
        full_kernel,
        grid=(chunks,),
        out_shape=jax.ShapeDtypeStruct((batch, length, 2 * rows, LANES), jnp.bfloat16),
        in_specs=[whole] * 3,
        out_specs=pl.BlockSpec((batch, steps, 2 * rows, LANES), lambda i: (0, i, 0, 0)),
        compiler_params=pltpu.CompilerParams(vmem_limit_bytes=GRANT),
        name="full",
    )(states, table, entry)
    return join_view(out)


def solution(mesh):
    in_specs = (P(None, "seq", None, "chan"), P("chan"), P("chan"), P())
    out_specs = P(None, "seq", None, "chan")
    return jax.shard_map(shards, mesh=mesh, in_specs=in_specs, out_specs=out_specs, check_vma=False)
```

```python
import functools

import jax
import jax.numpy as jnp
from jax import lax
from jax.experimental import pallas as pl
from jax.experimental.pallas import tpu as pltpu
from jax.sharding import PartitionSpec as P

LANES = 128
GRANT = 12 * 1024 * 1024


def coefficients(decay_rate, phase):
    magnitude = jnp.exp(-decay_rate)
    y = 2.0 * decay_rate
    series = 1.0 - y / 6.0 * (1.0 - y / 7.0)
    for n in (5.0, 4.0, 3.0, 2.0):
        series = 1.0 - y / n * series
    gamma = jnp.sqrt(jnp.where(y < 0.0625, y * series, 1.0 - jnp.exp(-y)))
    return (magnitude * jnp.cos(phase), magnitude * jnp.sin(phase), gamma)


def split_view(x):
    b, t, _, c = x.shape
    x = x.reshape(b, t, 2, c // LANES, LANES)
    return x.transpose(0, 1, 3, 2, 4).reshape(b, t, 2 * c // LANES, LANES)


def join_view(x):
    b, t, r, _ = x.shape
    x = x.reshape(b, t, r // 2, 2, LANES)
    return x.transpose(0, 1, 3, 2, 4).reshape(b, t, 2, r * LANES // 2)


def scan_chunk(keep, base, src, lre, lim, gam, state, store):
    batch, steps, rows2, _ = src.shape
    rows = rows2 // 2
    even = pl.ds(0, rows, stride=2)
    odd = pl.ds(1, rows, stride=2)
    for t in range(steps):
        for s in range(batch):
            hre, him = state[s]
            k = keep[s, base + t]
            hre, him = hre * k, him * k
            xre = src[s, t, even, :]
            xim = src[s, t, odd, :]
            if gam is not None:
                xre, xim = xre * gam, xim * gam
            nre = lre * hre - lim * him + xre
            nim = lre * him + lim * hre + xim
            state[s] = (nre, nim)
            if store:
                src[s, t, even, :] = nre
                src[s, t, odd, :] = nim
    return state


def cmul(a, b):
    return a[0] * b[0] - a[1] * b[1], a[0] * b[1] + a[1] * b[0]


def exchange(length, group, blocks, keep_rows, coef, prods, span, own, near, total, far, spread, back, sems, carry, fill_a, fill_b):
    send_a, recv_a, send_b, recv_b, send_c, recv_c = sems
    batch = own.shape[2]
    me = lax.axis_index("seq")
    part = lax.rem(me, group)
    at = me // group
    groups = blocks // group

    def member(d):
        return lax.rem(part + d, group)

    def copy(src, dst, send, recv, target):
        return pltpu.make_async_remote_copy(
            src_ref=src, dst_ref=dst, send_sem=send, recv_sem=recv,
            device_id={"seq": target}, device_id_type=pl.DeviceIdType.MESH,
        )

    def copy_a(d):
        return copy(own.at[member(d)], near.at[d], send_a.at[d], recv_a.at[d], at * group + member(d))

    def copy_b(d):
        return copy(total, far.at[d], send_b.at[d], recv_b.at[d], me + d * group)

    def copy_c(d):
        return copy(spread.at[d], back.at[d], send_c.at[d], recv_c.at[d], at * group + member(d))

    for d in range(group - 1, 0, -1):
        copy_a(d).start()
    near[0] = own[part]
    power = (coef[0], coef[1])
    done, left = None, length
    while left:
        if left % 2:
            done = power if done is None else cmul(done, power)
        left //= 2
        if left:
            power = cmul(power, power)
    part_rows = own.shape[3]
    for p in range(group):
        for c in range(2):
            span[p, c] = done[c][p * part_rows : (p + 1) * part_rows]
    for b in range(blocks):
        logs = jnp.log(keep_rows[:, b * length : (b + 1) * length])
        prods[b] = jnp.broadcast_to(jnp.exp(jnp.sum(logs, axis=1, keepdims=True)), prods.shape[1:])
    lam = (span[part, 0], span[part, 1])
    fill_a()
    powers = [None, lam]
    for _ in range(group - 1):
        powers.append(cmul(powers[-1], lam))
    for d in range(1, group):
        copy_a(d).wait_recv()

    inner = [[None] * batch for _ in range(group + 1)]
    scales = [[None] * batch for _ in range(group + 1)]
    for i in range(group):
        slot = lax.rem(part + group - i, group)
        for s in range(batch):
            k = prods[at * group + i, pl.ds(s, 1), :]
            end = (near[slot, 0, s], near[slot, 1, s])
            if i == 0:
                inner[1][s], scales[1][s] = end, k
            else:
                step = cmul((k * lam[0], k * lam[1]), inner[i][s])
                inner[i + 1][s] = (step[0] + end[0], step[1] + end[1])
                scales[i + 1][s] = scales[i][s] * k
    for s in range(batch):
        total[0, s], total[1, s] = inner[group][s]
    for d in range(groups - 1, 0, -1):

        @pl.when(at + d < groups)
        def _(d=d):
            copy_b(d).start()

    for m in range(group):
        slot = lax.rem(m + group - part, group)
        for s in range(batch):
            if m == 0:
                zero = jnp.zeros_like(lam[0])
                spread[slot, 0, s], spread[slot, 1, s] = zero, zero
            else:
                spread[slot, 0, s], spread[slot, 1, s] = inner[m][s]
    far[0] = jnp.zeros(far.shape[1:], jnp.float32)
    fill_b()
    for d in range(groups - 1, 0, -1):

        @pl.when(at - d >= 0)
        def _(d=d):
            copy_b(d).wait_recv()
            for s in range(batch):
                k = prods[(at - d) * group, pl.ds(s, 1), :]
                for i in range(1, group):
                    k = k * prods[(at - d) * group + i, pl.ds(s, 1), :]
                step = cmul((k * powers[group][0], k * powers[group][1]), (far[0, 0, s], far[0, 1, s]))
                far[0, 0, s] = step[0] + far[d, 0, s]
                far[0, 1, s] = step[1] + far[d, 1, s]

    entry = [(far[0, 0, s], far[0, 1, s]) for s in range(batch)]
    for m in range(group):
        slot = lax.rem(m + group - part, group)
        for s in range(batch):
            if m == 0:
                step = entry[s]
            else:
                step = cmul((scales[m][s] * powers[m][0], scales[m][s] * powers[m][1]), entry[s])
            spread[slot, 0, s] += step[0]
            spread[slot, 1, s] += step[1]
    for d in range(group - 1, 0, -1):
        copy_c(d).start()
    carry[part] = spread[0]
    for d in range(1, group):
        copy_c(d).wait_recv()
        carry[lax.rem(part + group - d, group)] = back[d]
    for d in range(1, group):
        copy_a(d).wait_send()
        copy_c(d).wait_send()
    for d in range(1, groups):

        @pl.when(at + d < groups)
        def _(d=d):
            copy_b(d).wait_send()


def end_kernel(length, group, blocks, steps, keep_hbm, x, decay_hbm, phase_hbm, states, table, entry,
               keep, keep_rows, decay, phase, coef, twice, prods, span, own, near, total, far, spread, back, carry,
               small_sem, *sems):
    batch = states.shape[0]
    rows = coef.shape[1]
    chunks = length // steps
    even = pl.ds(0, rows, stride=2)
    odd = pl.ds(1, rows, stride=2)
    small = [
        pltpu.make_async_copy(src, dst, small_sem.at[i])
        for i, (src, dst) in enumerate(
            ((decay_hbm, decay), (phase_hbm, phase), (keep_hbm, keep), (keep_hbm, keep_rows))
        )
    ]

    for copy in small:
        copy.start()

    me = lax.axis_index("seq")
    barrier = pltpu.get_barrier_semaphore()
    first = me // group * group
    for d in range(1, group):
        peer = first + lax.rem(me + d, group)
        pl.semaphore_signal(barrier, inc=1, device_id={"seq": peer}, device_id_type=pl.DeviceIdType.MESH)
    for d in range(1, blocks // group):
        peer = lax.rem(me + d * group, blocks)
        pl.semaphore_signal(barrier, inc=1, device_id={"seq": peer}, device_id_type=pl.DeviceIdType.MESH)

    small[0].wait()
    small[1].wait()
    coef[0], coef[1], coef[2] = coefficients(decay[...], phase[...])
    for c in range(2):
        twice[c, even, :] = coef[c]
        twice[c, odd, :] = coef[c]
    small[2].wait()
    base = me * length
    zero = jnp.zeros((rows, LANES), jnp.float32)
    start = tuple((zero, zero) for _ in range(batch))

    def ends(i, state):
        at = pl.ds(i * steps, steps)
        states[:, at] = x[:, at].astype(jnp.float32)
        state = scan_chunk(keep, base + i * steps, states.at[:, at], coef[0], coef[1], None, list(state), False)
        return tuple(state)

    state = lax.fori_loop(0, chunks, ends, start)
    part_rows = own.shape[3]
    for s in range(batch):
        for c in range(2):
            value = state[s][c] * coef[2]
            for p in range(group):
                own[p, c, s] = value[p * part_rows : (p + 1) * part_rows]

    def fill_a():
        ones = jnp.ones((2 * rows, LANES), jnp.float32)

        def powers(i, held):
            power, scale = held
            scale = list(scale)
            for t in range(4):
                power = cmul((twice[0], twice[1]), power)
                for s in range(batch):
                    scale[s] = scale[s] * keep[s, base + i * 4 + t]
                    table[s, i * 4 + t, 0] = scale[s] * power[0]
                    table[s, i * 4 + t, 1] = scale[s] * power[1]
            return power, tuple(scale)

        unit = tuple(jnp.float32(1) for _ in range(batch))
        lax.fori_loop(0, length // 4, powers, ((ones, jnp.zeros_like(ones)), unit))

    def fill_b():
        def local(i, state):
            at = pl.ds(i * steps, steps)
            view = states.at[:, at]
            return tuple(scan_chunk(keep, base + i * steps, view, coef[0], coef[1], coef[2], list(state), True))

        lax.fori_loop(0, chunks, local, start)

    small[3].wait()
    pl.semaphore_wait(barrier, group - 1 + blocks // group - 1)
    exchange(length, group, blocks, keep_rows, coef, prods, span, own, near, total, far, spread, back, sems, carry,
             fill_a, fill_b)
    for s in range(batch):
        for p in range(group):
            top = pl.ds(2 * p * part_rows, part_rows, stride=2)
            low = pl.ds(2 * p * part_rows + 1, part_rows, stride=2)
            entry[s, 0, top, :] = carry[p, 0, s]
            entry[s, 0, low, :] = carry[p, 1, s]
            entry[s, 1, top, :] = -carry[p, 1, s]
            entry[s, 1, low, :] = carry[p, 0, s]


def full_kernel(states, table, entry, out):
    batch, steps = out.shape[:2]
    base = pl.program_id(0) * steps
    for s in range(batch):
        for t in range(steps):
            at = base + t
            moved = table[s, at, 0] * entry[s, 0] + table[s, at, 1] * entry[s, 1]
            out[s, t] = (states[s, at] + moved).astype(jnp.bfloat16)


def shards(inputs, decay_rate, phase, keep):
    batch, length, _, width = inputs.shape
    rows = width // LANES
    x = split_view(inputs)
    steps = min(16, length)
    chunks = length // steps
    blocks = lax.axis_size("seq")
    group = 4
    groups = blocks // group
    whole = pl.BlockSpec(memory_space=pltpu.VMEM)
    away = pl.BlockSpec(memory_space=pltpu.HBM)
    piece = (2, batch, rows // group, LANES)
    dma = pltpu.SemaphoreType.DMA
    f32 = jnp.float32
    states, table, entry = pl.pallas_call(
        functools.partial(end_kernel, length, group, blocks, steps),
        out_shape=(
            jax.ShapeDtypeStruct((batch, length, 2 * rows, LANES), f32),
            jax.ShapeDtypeStruct((batch, length, 2, 2 * rows, LANES), f32),
            jax.ShapeDtypeStruct((batch, 2, 2 * rows, LANES), f32),
        ),
        in_specs=[away, whole, away, away],
        out_specs=(whole,) * 3,
        scratch_shapes=[
            pltpu.SMEM(keep.shape, f32),
            pltpu.VMEM(keep.shape, f32),
            pltpu.VMEM((rows, LANES), f32),
            pltpu.VMEM((rows, LANES), f32),
            pltpu.VMEM((3, rows, LANES), f32),
            pltpu.VMEM((2, 2 * rows, LANES), f32),
            pltpu.VMEM((blocks, batch, LANES), f32),
            pltpu.VMEM((group, 2, rows // group, LANES), f32),
            pltpu.VMEM((group,) + piece, f32),
            pltpu.VMEM((group,) + piece, f32),
            pltpu.VMEM(piece, f32),
            pltpu.VMEM((groups,) + piece, f32),
            pltpu.VMEM((group,) + piece, f32),
            pltpu.VMEM((group,) + piece, f32),
            pltpu.VMEM((group,) + piece, f32),
            dma((4,)),
            dma((group,)), dma((group,)), dma((groups,)), dma((groups,)), dma((group,)), dma((group,)),
        ],
        compiler_params=pltpu.CompilerParams(collective_id=0, has_side_effects=True, vmem_limit_bytes=GRANT),
        name="ends",
    )(keep, x, decay_rate.reshape(rows, LANES), phase.reshape(rows, LANES))
    out = pl.pallas_call(
        full_kernel,
        grid=(chunks,),
        out_shape=jax.ShapeDtypeStruct((batch, length, 2 * rows, LANES), jnp.bfloat16),
        in_specs=[whole] * 3,
        out_specs=pl.BlockSpec((batch, steps, 2 * rows, LANES), lambda i: (0, i, 0, 0)),
        compiler_params=pltpu.CompilerParams(vmem_limit_bytes=GRANT),
        name="full",
    )(states, table, entry)
    return join_view(out)


def solution(mesh):
    in_specs = (P(None, "seq", None, "chan"), P("chan"), P("chan"), P())
    out_specs = P(None, "seq", None, "chan")
    return jax.shard_map(shards, mesh=mesh, in_specs=in_specs, out_specs=out_specs, check_vma=False)
```
